32 devices in a mesh: fsdp: 4 (over y, core), sp: 8 (over z, x).
Axes of the slice: x: 2, y: 2, z: 4, core: 2. Of those that a mesh axis runs over, the one named last changes fastest.
Arguments:
- hidden: bfloat16 [4, 2048, 5120], P('fsdp', 'sp'), may hold values from -6 to 6
- queries: bfloat16 [4, 2048, 4096], P('fsdp', 'sp'), may hold values from -240 to 240
- norm_gain: float32 [5120], replicated, may hold values from 0.5 to 1.5
- kv_weight: bfloat16 [5120, 2048], P('fsdp'), may hold values from -0.078125 to 0.078125
- value_bias: float32 [1024], replicated, may hold values from -3 to 3
- doc_lengths: int32 [4, 16], P('fsdp'), may hold values from 1 to 512, 2048 in all within a row
Outputs:
- attended: bfloat16 [4, 2048, 4096], P('fsdp', 'sp')
The draws below stay inside these ranges and needn't reach their ends.
Inputs may be any that keep to these rules, and one draw needn't show every extreme that they name: `doc_lengths`: each row sums to 2048 and its largest entry is 512.
All inputs are finite; a program needn't handle non-finite values.
Results may differ from the reference program's by a relative error of at most 0.0067.
Values may be sent and summed in bfloat16 or wider, within the bound.
No kernel may reach another device: no remote copies, remote signals or barrier semaphores. Data moves between devices by JAX's collectives and lax.ppermute only.
A program may use at most 128 MiB of HBM per device.

```python
import math
import jax
import jax.numpy as jnp
import numpy as np
from jax import lax

D = 5120
QH = 32
KVH = 8
HD = 128
NDOC = 16
GROUPS = 4
SEQ = 2048
MOST = 512


def draw_queries(key, part):
    drawn = jnp.clip(jax.random.normal(key, (GROUPS, SEQ, QH * HD), jnp.float32), -6.0, 6.0)
    return drawn.astype(jnp.bfloat16)


def steps_of(rng, extent, shards, low, high):
    loudness, own = 1.0, jax.random.fold_in(rng, 6)
    for position, parts in shards:
        steps = jnp.exp(jax.random.uniform(jax.random.fold_in(own, position), (parts,), jnp.float32, low / len(shards), high / len(shards)))
        loudness = loudness * jnp.repeat(steps, extent[position] // parts).reshape([-1 if axis == position else 1 for axis in range(len(extent))])
    return loudness


def split_up(number_of, total, bound, lean):
    portions = [(1 << 20) // math.isqrt(standing ** lean) + 1 for standing in range(2, number_of + 1)]
    spare, given = total - bound - (number_of - 1), [1] * (number_of - 1)
    while spare > 0:
        movable = [i for i in range(number_of - 1) if given[i] < bound]
        whole, remaining = sum([portions[i] for i in movable]), spare
        for i in movable:
            addition = min(bound - given[i], max(1, remaining * portions[i] // whole), spare)
            given[i] = given[i] + addition
            spare = spare - addition
    return np.array([bound] + given)


def uneven(key, count, total, reach, skew):
    if count == 2:
        one = jax.random.randint(key, (), max(1, total - reach), min(reach, total - 1) + 1)
        return jnp.stack([one, total - one])
    sizes = jnp.asarray(split_up(count, total, reach, skew), jnp.int32)
    couples = (count - 1) // 2
    donor, taker = sizes[1:1 + 2 * couples:2], sizes[2:2 + 2 * couples:2]
    room = jnp.minimum(donor - 1, reach - taker)
    shifted = jax.random.randint(jax.random.fold_in(key, 1), (couples,), 0, 1 << 20) % (room + 1)
    sizes = sizes.at[1:1 + 2 * couples:2].set(donor - shifted).at[2:2 + 2 * couples:2].set(taker + shifted)
    return sizes[jax.random.permutation(jax.random.fold_in(key, 2), count)]


def gaussian(key, shape, width, most, cuts=(), kind=jnp.bfloat16):
    values = jax.random.normal(key, shape, jnp.float32) * width
    if len(cuts) > 0:
        values = steps_of(key, shape, cuts, -0.22, 0.18) * values
    return jnp.clip(values, min=-most, max=most).astype(kind)


def setup_inputs(seed: int = 0) -> dict:
    seeds = jax.random.split(jax.random.key(seed), 7)
    hidden = gaussian(seeds[0], (GROUPS, SEQ, D), 1.0, 6.0, ((0, 4), (1, 8)))
    queries = draw_queries(jax.random.fold_in(seeds[6], 71), 0)
    norm_gain = jnp.clip(1.0 + 0.1 * jax.random.normal(seeds[2], (D,), jnp.float32), 0.5, 1.5)
    kv_weight = gaussian(seeds[3], (D, 2 * KVH * HD), D ** -0.5, 0.078125, ((0, 4),))
    value_bias = gaussian(seeds[4], (KVH * HD,), 0.5, 3.0, (), jnp.float32)
    doc_lengths = jax.vmap(lambda own: uneven(own, NDOC, SEQ, MOST, 2))(jax.random.split(seeds[5], GROUPS)).reshape((GROUPS, NDOC)).astype(jnp.int32)
    return {"hidden": hidden, "queries": queries, "norm_gain": norm_gain, "kv_weight": kv_weight, "value_bias": value_bias, "doc_lengths": doc_lengths}


EPS = 1e-06

def attend(query_all, key_all, value_all, doc_ids):
    length = query_all.shape[0]
    block = min(512, length)
    longest = length // 4
    window = min(length, block + longest)
    scale = HD ** (-0.5)

    def one_block(index):
        first = (index * block).astype(jnp.int32)
        start = jnp.clip(first - longest, 0, length - window).astype(jnp.int32)
        query_block = lax.dynamic_slice_in_dim(query_all, first, block, 0).astype(jnp.float32)
        key_block = lax.dynamic_slice_in_dim(key_all, start, window, 0).astype(jnp.float32)
        value_block = lax.dynamic_slice_in_dim(value_all, start, window, 0).astype(jnp.float32)
        query_ids = lax.dynamic_slice_in_dim(doc_ids, first, block, 0)
        key_ids = lax.dynamic_slice_in_dim(doc_ids, start, window, 0)
        query_pos = first + jnp.arange(block, dtype=jnp.int32)
        key_pos = start + jnp.arange(window, dtype=jnp.int32)
        allowed = (key_pos[None, :] <= query_pos[:, None]) & (key_ids[None, :] == query_ids[:, None])
        scores = jnp.einsum('qnd,knd->nqk', query_block, key_block) * scale
        scores = jnp.where(allowed[None], scores, -jnp.inf)
        highest = lax.optimization_barrier(jnp.max(scores, axis=-1, keepdims=True))
        probs = jnp.exp(scores - highest)
        probs = (probs / lax.optimization_barrier(jnp.sum(probs, axis=-1, keepdims=True))).astype(jnp.bfloat16)
        output = jnp.einsum('nqk,knd->qnd', probs.astype(jnp.float32), value_block)
        return output.astype(jnp.bfloat16)
    blocks = lax.map(one_block, jnp.arange(length // block, dtype=jnp.int32))
    return blocks.reshape(length, query_all.shape[1], query_all.shape[2])

def reference(hidden, queries, norm_gain, kv_weight, value_bias, doc_lengths):
    wide = hidden.astype(jnp.float32)
    normed = (wide * lax.rsqrt(lax.optimization_barrier(jnp.mean(wide * wide, axis=-1, keepdims=True)) + EPS) * norm_gain).astype(jnp.bfloat16)
    projected = jnp.dot(normed.reshape(GROUPS * SEQ, D), kv_weight, preferred_element_type=jnp.float32)
    projected = projected.reshape(GROUPS, SEQ, 2 * KVH * HD)
    keys = projected[..., :KVH * HD].astype(jnp.bfloat16)
    values = (projected[..., KVH * HD:] + value_bias).astype(jnp.bfloat16)
    ratio = QH // KVH

    def one_group(operands):
        query_group, key_group, value_group, lengths = operands
        ends = jnp.cumsum(lengths).astype(jnp.int32)
        positions = jnp.arange(SEQ, dtype=jnp.int32)
        doc_ids = lax.optimization_barrier(jnp.sum((positions[:, None] >= ends[None, :]).astype(jnp.int32), axis=1)).astype(jnp.int32)
        query_heads = query_group.reshape(SEQ, QH, HD)
        key_heads = jnp.repeat(key_group.reshape(SEQ, KVH, HD), ratio, axis=1)
        value_heads = jnp.repeat(value_group.reshape(SEQ, KVH, HD), ratio, axis=1)
        return attend(query_heads, key_heads, value_heads, doc_ids).reshape(SEQ, QH * HD)
    return lax.map(one_group, (queries, keys, values, doc_lengths))
```

```python
import functools

import jax
import jax.numpy as jnp
from jax import lax
from jax.experimental import pallas as pl
from jax.experimental.pallas import tpu as pltpu
from jax.sharding import PartitionSpec as P

QH = 32
KVH = 8
HD = 128
EPS = 1e-06
RATIO = QH // KVH
LOG2E = 1.4426950408889634
CHUNKS = 4
TILE = 128
HIDDEN = -1e30


def project_kernel(rows_ref, own_ref, other_ref, out_ref):
    depth = own_ref.shape[0]
    total = jnp.dot(rows_ref[:, :depth], own_ref[...], preferred_element_type=jnp.float32)
    total += jnp.dot(rows_ref[:, depth:], other_ref[...], preferred_element_type=jnp.float32)
    out_ref[...] = total.astype(out_ref.dtype)


def project(rows, weight_own, weight_other, chunk, heads, dtype):
    tokens, depth = rows.shape
    width = heads * HD
    chunks = KVH // heads
    held = weight_own.shape[0]
    spec = pl.BlockSpec((held, width), lambda i: (0, i * chunks + chunk))
    return pl.pallas_call(
        project_kernel,
        grid=(2,),
        in_specs=[pl.BlockSpec((tokens, depth), lambda i: (0, 0)), spec, spec],
        out_specs=pl.BlockSpec((tokens, width), lambda i: (0, i)),
        out_shape=jax.ShapeDtypeStruct((tokens, 2 * width), dtype),
        cost_estimate=pl.CostEstimate(
            flops=4 * tokens * depth * width,
            bytes_accessed=4 * depth * width + 2 * tokens * depth,
            transcendentals=0,
        ),
        name="project",
    )(rows, weight_own, weight_other)


def attend_kernel(reach, first_out, lengths_ref, query_ref, *refs):
    blocks = reach + 1
    keys, values = refs[:blocks], refs[blocks : 2 * blocks]
    out_ref, bias = refs[-2], refs[-1]
    tokens = query_ref.shape[0]
    window = blocks * tokens
    first = lax.axis_index("sp") * tokens

    @pl.when(pl.program_id(0) == 0)
    def _():
        query_pos = first + lax.broadcasted_iota(jnp.int32, (tokens, TILE), 0)
        start = jnp.zeros((tokens, TILE), jnp.int32)
        end = jnp.int32(0)
        for i in range(lengths_ref.shape[1]):
            end = end + lengths_ref[0, i]
            start = jnp.where(query_pos >= end, end, start)
        for j in range(0, window, TILE):
            key_pos = (
                first - reach * tokens + j + lax.broadcasted_iota(jnp.int32, (tokens, TILE), 1)
            )
            allowed = (key_pos >= start) & (key_pos <= query_pos)
            bias[:, j : j + TILE] = jnp.where(allowed, 0.0, HIDDEN).astype(jnp.float32)

    scale = HD ** (-0.5) * LOG2E
    for t in range(0, tokens, TILE):
        low, high = t, t + reach * tokens + TILE
        queries = jnp.concatenate(
            [query_ref[t : t + TILE, h * HD : (h + 1) * HD] for h in range(RATIO)], axis=0
        )
        spans = []
        for b in range(blocks):
            a, z = max(low - b * tokens, 0), min(high - b * tokens, tokens)
            if a < z:
                spans.append((b, a, z))
        scores = jnp.concatenate(
            [
                lax.dot_general(
                    queries,
                    keys[b][a:z, :],
                    (((1,), (1,)), ((), ())),
                    preferred_element_type=jnp.float32,
                )
                for b, a, z in spans
            ],
            axis=1,
        )
        mask = bias[t : t + TILE, low:high]
        scores = scores * scale + jnp.concatenate([mask] * RATIO, axis=0)
        highest = jnp.max(scores, axis=1, keepdims=True)
        probs = jnp.exp2(scores - highest).astype(jnp.bfloat16)
        total = jnp.zeros((RATIO * TILE, 2 * HD), jnp.float32)
        for b, a, z in spans:
            at = b * tokens + a - low
            value = jnp.concatenate(
                [values[b][a:z, :], jnp.ones((z - a, HD), jnp.bfloat16)], axis=1
            )
            total += jnp.dot(
                probs[:, at : at + z - a], value, preferred_element_type=jnp.float32
            )
        result = (total[:, :HD] / total[:, HD:]).astype(out_ref.dtype)
        for h in range(RATIO):
            out_ref[t : t + TILE, h * HD : (h + 1) * HD] = result[h * TILE : (h + 1) * TILE]


def attend(lengths, queries, blocks, chunk, heads, partial):
    tokens = queries.shape[0]
    reach = len(blocks) - 1
    in_specs = [
        pl.BlockSpec(memory_space=pltpu.SMEM),
        pl.BlockSpec((tokens, RATIO * HD), lambda i: (0, chunk * heads + i)),
    ]
    in_specs += [pl.BlockSpec((tokens, HD), lambda i: (0, i))] * len(blocks)
    in_specs += [pl.BlockSpec((tokens, HD), lambda i: (0, heads + i))] * len(blocks)
    operands = [lengths, queries, *blocks, *blocks]
    aliases = {}
    if partial is not None:
        aliases = {len(operands): 0}
        operands.append(partial)
        in_specs.append(pl.BlockSpec(memory_space=pl.ANY))
    keys = tokens * (reach + 1)
    return pl.pallas_call(
        functools.partial(attend_kernel, reach, partial is None),
        grid=(heads,),
        in_specs=in_specs,
        out_specs=pl.BlockSpec((tokens, RATIO * HD), lambda i: (0, chunk * heads + i)),
        out_shape=jax.ShapeDtypeStruct((tokens, QH * HD), jnp.bfloat16),
        scratch_shapes=[pltpu.VMEM((tokens, keys), jnp.float32)],
        input_output_aliases=aliases,
        cost_estimate=pl.CostEstimate(
            flops=6 * heads * RATIO * tokens * keys * HD,
            bytes_accessed=4 * tokens * heads * (RATIO + reach + 1) * HD,
            transcendentals=heads * RATIO * tokens * keys,
        ),
        name="attend",
    )(*operands)


def shards(hidden, queries, norm_gain, kv_weight, value_bias, doc_lengths):
    tokens = hidden.shape[1]
    parts = lax.axis_size("fsdp")
    length = lax.axis_size("sp")
    held = kv_weight.shape[0]
    pair = 2 if parts % 2 == 0 else 1
    groups = parts // pair
    me = lax.axis_index("fsdp")
    place = lax.axis_index("sp")
    group, core = me // pair, me % pair
    reach = length // 4
    heads = KVH // CHUNKS
    width = heads * HD

    wide = hidden[0].astype(jnp.float32)
    power = lax.rsqrt(jnp.mean(wide * wide, axis=-1, keepdims=True) + EPS)

    def normed(whose):
        def part(quarter):
            rows = lax.dynamic_slice_in_dim(hidden[0], quarter * held, held, 1)
            gain = lax.dynamic_slice_in_dim(norm_gain, quarter * held, held, 0)
            return (rows.astype(jnp.float32) * power * gain).astype(jnp.bfloat16)

        quarters = [whose * pair + core, whose * pair + (pair - 1 - core)]
        return jnp.concatenate([part(q) for q in quarters[:pair]], axis=1)

    arrived = []
    for d in range(1, groups):
        there = [(i, (i + d * pair) % parts) for i in range(parts)]
        arrived.append(lax.ppermute(normed((group + d) % groups), "fsdp", there))
    if pair == 2:
        weight_other = lax.ppermute(kv_weight, "fsdp", [(i, i ^ 1) for i in range(parts)])
    else:
        weight_other = jnp.zeros_like(kv_weight)
    mine = normed(group)
    if pair == 1:
        mine = jnp.concatenate([mine, jnp.zeros_like(mine)], axis=1)
        arrived = [jnp.concatenate([a, jnp.zeros_like(a)], axis=1) for a in arrived]

    out = None
    for c in range(CHUNKS):
        total = project(mine, kv_weight, weight_other, c, heads, jnp.float32)
        for d in range(1, groups):
            back = [(i, (i - d * pair) % parts) for i in range(parts)]
            part = project(arrived[d - 1], kv_weight, weight_other, c, heads, jnp.bfloat16)
            total = total + lax.ppermute(part, "fsdp", back).astype(jnp.float32)
        bias = lax.dynamic_slice_in_dim(value_bias, c * width, width, 0)
        total = total + jnp.concatenate([jnp.zeros_like(bias), bias])
        own = total.astype(jnp.bfloat16)
        blocks = [own]
        if reach % 2 == 0 and length % 2 == 0:
            far = []
            for b in range(2, reach + 1, 2):
                far.append(lax.ppermute(own, "sp", [(i, i + b) for i in range(length - b)]))
            swap = [(i, i ^ 1) for i in range(length)]
            odd = place % 2 == 1
            chain = [own] + far
            near = [
                lax.ppermute(jnp.where(odd, chain[b + 1], chain[b]), "sp", swap)
                for b in range(reach // 2)
            ]
            for b in range(reach // 2):
                blocks = [far[b], near[b]] + blocks
        else:
            for b in range(1, reach + 1):
                blocks = [
                    lax.ppermute(own, "sp", [(i, i + b) for i in range(length - b)])
                ] + blocks
        out = attend(doc_lengths, queries[0], blocks, c, heads, out)
    return out.reshape(1, tokens, QH * HD)


def solution(mesh):
    in_specs = (
        P("fsdp", "sp", None),
        P("fsdp", "sp", None),
        P(),
        P("fsdp", None),
        P(),
        P("fsdp", None),
    )
    out_specs = P("fsdp", "sp", None)
    return jax.shard_map(shards, mesh=mesh, in_specs=in_specs, out_specs=out_specs, check_vma=False)
```

```python
import functools

import jax
import jax.numpy as jnp
from jax import lax
from jax.experimental import pallas as pl
from jax.experimental.pallas import tpu as pltpu
from jax.sharding import PartitionSpec as P

QH = 32
KVH = 8
HD = 128
EPS = 1e-06
RATIO = QH // KVH
LOG2E = 1.4426950408889634
CHUNKS = 4
TILE = 128
HIDDEN = -1e30
MIB = 1 << 20
VMEM = pl.BlockSpec(memory_space=pltpu.VMEM)


def place_in(pair):
    me = lax.axis_index("fsdp")
    return lax.div(me, jnp.int32(pair)), lax.rem(me, jnp.int32(pair))


def scale_part(hidden_ref, gain_ref, out_ref, quarter, slot, held):
    columns = pl.ds(pl.multiple_of(quarter * held, HD), held)
    rows = hidden_ref[:, columns].astype(jnp.float32) * gain_ref[:, columns]
    out_ref[:, slot * held : (slot + 1) * held] = rows.astype(jnp.bfloat16)


def away_kernel(parts, pair, ahead, hidden_ref, gain_ref, out_ref):
    group, core = place_in(pair)
    there = lax.rem(group + ahead, jnp.int32(parts // pair)) * pair
    held = out_ref.shape[1] // pair
    scale_part(hidden_ref, gain_ref, out_ref, there + core, 0, held)
    if pair == 2:
        scale_part(hidden_ref, gain_ref, out_ref, there + 1 - core, 1, held)


def home_kernel(pair, hidden_ref, gain_ref, out_ref, power_ref):
    group, core = place_in(pair)
    held = out_ref.shape[1] // pair
    scale_part(hidden_ref, gain_ref, out_ref, group * pair + core, 0, held)
    if pair == 2:
        scale_part(hidden_ref, gain_ref, out_ref, group * pair + 1 - core, 1, held)
    tokens, model = hidden_ref.shape
    total = jnp.zeros((tokens, HD), jnp.float32)
    for j in range(0, model, HD):
        wide = hidden_ref[:, j : j + HD].astype(jnp.float32)
        total += wide * wide
    mean = jnp.sum(total, axis=1, keepdims=True) / model
    power_ref[...] = lax.rsqrt(mean + EPS)


def scaled(kernel, hidden, gain, width, powers):
    tokens = hidden.shape[0]
    out_shape = [jax.ShapeDtypeStruct((tokens, width), jnp.bfloat16)]
    if powers:
        out_shape.append(jax.ShapeDtypeStruct((tokens, 1), jnp.float32))
    return pl.pallas_call(
        kernel,
        in_specs=[VMEM, VMEM],
        out_specs=[VMEM] * len(out_shape),
        out_shape=out_shape,
        compiler_params=pltpu.CompilerParams(vmem_limit_bytes=16 * MIB),
        cost_estimate=pl.CostEstimate(
            flops=4 * tokens * width, bytes_accessed=4 * tokens * width, transcendentals=0
        ),
        name="scaled",
    )(hidden, gain)


def project_kernel(starts, width, rows_ref, *refs):
    weights, out_ref = refs[:-1], refs[-1]
    depth = weights[0].shape[0]
    for i, start in enumerate(starts):
        total = None
        for w, weight in enumerate(weights):
            term = jnp.dot(
                rows_ref[:, w * depth : (w + 1) * depth],
                weight[:, start : start + width],
                preferred_element_type=jnp.float32,
            )
            total = term if total is None else total + term
        out_ref[:, i * width : (i + 1) * width] = total.astype(out_ref.dtype)


def project(rows, weights, chunks, heads, dtype):
    tokens, depth = rows.shape
    width = heads * HD
    starts = [half * KVH * HD + c * width for c in chunks for half in range(2)]
    columns = len(starts) * width
    return pl.pallas_call(
        functools.partial(project_kernel, starts, width),
        in_specs=[VMEM] * (1 + len(weights)),
        out_specs=VMEM,
        out_shape=jax.ShapeDtypeStruct((tokens, columns), dtype),
        compiler_params=pltpu.CompilerParams(vmem_limit_bytes=24 * MIB),
        cost_estimate=pl.CostEstimate(
            flops=2 * tokens * depth * columns,
            bytes_accessed=2 * depth * columns,
            transcendentals=0,
        ),
        name="project",
    )(rows, *weights)


def merge_kernel(chunk, heads, home_ref, power_ref, bias_ref, *refs):
    parts, out_ref = refs[:-1], refs[-1]
    width = heads * HD
    total = home_ref[:, 2 * chunk * width : 2 * (chunk + 1) * width]
    for part in parts:
        total = total + part[...].astype(jnp.float32)
    total = total * power_ref[...]
    out_ref[:, :width] = total[:, :width].astype(jnp.bfloat16)
    bias = bias_ref[:, chunk * width : (chunk + 1) * width]
    out_ref[:, width:] = (total[:, width:] + bias).astype(jnp.bfloat16)


def merge(home, power, bias, parts, chunk, heads):
    tokens = home.shape[0]
    return pl.pallas_call(
        functools.partial(merge_kernel, chunk, heads),
        in_specs=[VMEM] * (3 + len(parts)),
        out_specs=VMEM,
        out_shape=jax.ShapeDtypeStruct((tokens, 2 * heads * HD), jnp.bfloat16),
        compiler_params=pltpu.CompilerParams(vmem_limit_bytes=4 * MIB),
        name="merge",
    )(home, power, bias, *parts)


def pick_kernel(even_ref, odd_ref, out_ref):
    odd = lax.rem(lax.axis_index("sp"), jnp.int32(2)) == 1

    @pl.when(odd)
    def _():
        out_ref[...] = odd_ref[...]

    @pl.when(jnp.logical_not(odd))
    def _():
        out_ref[...] = even_ref[...]


def pick(even, odd):
    return pl.pallas_call(
        pick_kernel,
        in_specs=[VMEM] * 2,
        out_specs=VMEM,
        out_shape=jax.ShapeDtypeStruct(even.shape, even.dtype),
        compiler_params=pltpu.CompilerParams(vmem_limit_bytes=4 * MIB),
        name="pick",
    )(even, odd)


def attend_kernel(reach, lengths_ref, query_ref, *refs):
    blocks = refs[: reach + 1]
    out_ref, bias = refs[-2], refs[-1]
    tokens = query_ref.shape[0]
    heads = blocks[0].shape[1] // (2 * HD)
    window = (reach + 1) * tokens
    first = lax.axis_index("sp") * tokens
    query_pos = first + lax.broadcasted_iota(jnp.int32, (tokens, TILE), 0)
    start = jnp.zeros((tokens, TILE), jnp.int32)
    end = jnp.int32(0)
    for i in range(lengths_ref.shape[1]):
        end = end + lengths_ref[0, i]
        start = jnp.where(query_pos >= end, end, start)
    for j in range(0, window, TILE):
        key_pos = first - reach * tokens + j + lax.broadcasted_iota(jnp.int32, (tokens, TILE), 1)
        allowed = (key_pos >= start) & (key_pos <= query_pos)
        bias[:, j : j + TILE] = jnp.where(allowed, 0.0, HIDDEN).astype(jnp.float32)

    scale = HD ** (-0.5) * LOG2E
    for head in range(heads):
        for t in range(0, tokens, TILE):
            low, high = t, t + reach * tokens + TILE
            wide = head * RATIO * HD
            queries = jnp.concatenate(
                [
                    query_ref[t : t + TILE, wide + h * HD : wide + (h + 1) * HD]
                    for h in range(RATIO)
                ],
                axis=0,
            )
            spans = []
            for b in range(reach + 1):
                a, z = max(low - b * tokens, 0), min(high - b * tokens, tokens)
                if a < z:
                    spans.append((b, a, z))
            scores = jnp.concatenate(
                [
                    lax.dot_general(
                        queries,
                        blocks[b][a:z, head * HD : (head + 1) * HD],
                        (((1,), (1,)), ((), ())),
                        preferred_element_type=jnp.float32,
                    )
                    for b, a, z in spans
                ],
                axis=1,
            )
            mask = bias[t : t + TILE, low:high]
            scores = scores * scale + jnp.concatenate([mask] * RATIO, axis=0)
            highest = jnp.max(scores, axis=1, keepdims=True)
            probs = jnp.exp2(scores - highest).astype(jnp.bfloat16)
            total = jnp.zeros((RATIO * TILE, 2 * HD), jnp.float32)
            for b, a, z in spans:
                at = b * tokens + a - low
                value = blocks[b][a:z, (heads + head) * HD : (heads + head + 1) * HD]
                value = jnp.concatenate([value, jnp.ones((z - a, HD), jnp.bfloat16)], axis=1)
                total += jnp.dot(
                    probs[:, at : at + z - a], value, preferred_element_type=jnp.float32
                )
            result = (total[:, :HD] / total[:, HD:]).astype(out_ref.dtype)
            for h in range(RATIO):
                out_ref[t : t + TILE, wide + h * HD : wide + (h + 1) * HD] = result[
                    h * TILE : (h + 1) * TILE
                ]


def attend(lengths, queries, blocks, chunk, heads, partial):
    tokens = queries.shape[0]
    reach = len(blocks) - 1
    width = heads * RATIO * HD
    columns = pl.BlockSpec((tokens, width), lambda i: (0, chunk))
    in_specs = [pl.BlockSpec(memory_space=pltpu.SMEM), columns] + [VMEM] * len(blocks)
    operands = [lengths, queries, *blocks]
    aliases = {}
    if partial is not None:
        aliases = {len(operands): 0}
        operands.append(partial)
        in_specs.append(pl.BlockSpec(memory_space=pl.ANY))
    keys = tokens * (reach + 1)
    return pl.pallas_call(
        functools.partial(attend_kernel, reach),
        grid=(1,),
        in_specs=in_specs,
        out_specs=columns,
        out_shape=jax.ShapeDtypeStruct((tokens, QH * HD), jnp.bfloat16),
        scratch_shapes=[pltpu.VMEM((tokens, keys), jnp.float32)],
        input_output_aliases=aliases,
        compiler_params=pltpu.CompilerParams(vmem_limit_bytes=24 * MIB),
        cost_estimate=pl.CostEstimate(
            flops=6 * heads * RATIO * tokens * keys * HD,
            bytes_accessed=4 * tokens * heads * (RATIO + reach + 1) * HD,
            transcendentals=heads * RATIO * tokens * keys,
        ),
        name="attend",
    )(*operands)


def shards(hidden, queries, norm_gain, kv_weight, value_bias, doc_lengths):
    return layer(hidden[0], queries[0], norm_gain, kv_weight, value_bias, doc_lengths)[None]


def layer(hidden, queries, norm_gain, kv_weight, value_bias, doc_lengths):
    parts = lax.axis_size("fsdp")
    length = lax.axis_size("sp")
    held = kv_weight.shape[0]
    pair = 2 if parts % 2 == 0 else 1
    groups = parts // pair
    reach = length // 4
    heads = KVH // CHUNKS
    gain = norm_gain[None]

    arrived = []
    for d in range(1, groups):
        there = [(i, (i + d * pair) % parts) for i in range(parts)]
        kernel = functools.partial(away_kernel, parts, pair, d)
        sent = scaled(kernel, hidden, gain, pair * held, False)[0]
        arrived.append(lax.ppermute(sent, "fsdp", there))
    weights = [kv_weight]
    if pair == 2:
        weights.append(lax.ppermute(kv_weight, "fsdp", [(i, i ^ 1) for i in range(parts)]))
    kernel = functools.partial(home_kernel, pair)
    mine, power = scaled(kernel, hidden, gain, pair * held, True)
    totals = project(mine, weights, range(CHUNKS), heads, jnp.float32)

    sums = []
    for c in range(CHUNKS):
        returned = []
        for d in range(1, groups):
            back = [(i, (i - d * pair) % parts) for i in range(parts)]
            part = project(arrived[d - 1], weights, [c], heads, jnp.bfloat16)
            returned.append(lax.ppermute(part, "fsdp", back))
        sums.append(merge(totals, power, value_bias[None], returned, c, heads))

    out = None
    for c, own in enumerate(sums):
        blocks = [own]
        if reach % 2 == 0 and length % 2 == 0:
            chain = [own]
            for b in range(2, reach + 1, 2):
                ahead = [(i, i + b) for i in range(length - b)]
                chain.append(lax.ppermute(own, "sp", ahead))
            swap = [(i, i ^ 1) for i in range(length)]
            for b in range(reach // 2):
                near = lax.ppermute(pick(chain[b], chain[b + 1]), "sp", swap)
                blocks = [chain[b + 1], near] + blocks
        else:
            for b in range(1, reach + 1):
                ahead = [(i, i + b) for i in range(length - b)]
                blocks = [lax.ppermute(own, "sp", ahead)] + blocks
        out = attend(doc_lengths, queries, blocks, c, heads, out)
    return out


def solution(mesh):
    in_specs = (
        P("fsdp", "sp", None),
        P("fsdp", "sp", None),
        P(),
        P("fsdp", None),
        P(),
        P("fsdp", None),
    )
    out_specs = P("fsdp", "sp", None)
    return jax.shard_map(shards, mesh=mesh, in_specs=in_specs, out_specs=out_specs, check_vma=False)
```

```python
import functools

import jax
import jax.numpy as jnp
from jax import lax
from jax.experimental import pallas as pl
from jax.experimental.pallas import tpu as pltpu
from jax.sharding import PartitionSpec as P

QH = 32
KVH = 8
HD = 128
EPS = 1e-06
RATIO = QH // KVH
LOG2E = 1.4426950408889634
SUMS = ((0, 1), (2, 3), (4, 5), (6, 7))
BLOCKS = ((0, 1), (2, 3), (4, 5), (6,), (7,))
PIECES = 2
TILE = 128
STRIP = 32
AHEAD = 2
MASKED = -1e30
MIB = 1 << 20
VMEM = pl.BlockSpec(memory_space=pltpu.VMEM)
SMEM = pl.BlockSpec(memory_space=pltpu.SMEM)
HBM = pl.BlockSpec(memory_space=pltpu.HBM)


def in_hbm(value):
    return pltpu.with_memory_space_constraint(value, pltpu.HBM)


def place_of(parts, pair, ahead, held):
    me = lax.axis_index("fsdp")
    group, core = lax.div(me, jnp.int32(pair)), lax.rem(me, jnp.int32(pair))
    there = lax.rem(group + ahead, jnp.int32(parts // pair))
    return pl.multiple_of(there * (pair * held), HD), core


def put_scaled(out_ref, rows_ref, gain_ref, some, core):
    held = out_ref.shape[1] // 2

    @pl.when(core == 0)
    def _():
        out_ref[...] = (rows_ref[some, :].astype(jnp.float32) * gain_ref[...]).astype(jnp.bfloat16)

    @pl.when(core == 1)
    def _():
        for a, b in ((0, held), (held, 0)):
            wide = rows_ref[some, a : a + held].astype(jnp.float32)
            scaled = wide * gain_ref[:, a : a + held]
            out_ref[:, b : b + held] = scaled.astype(jnp.bfloat16)


def away_kernel(parts, pair, ahead, piece, hidden_ref, gain_ref, out_ref, rows, gains, sems):
    step, width = rows.shape
    first, core = place_of(parts, pair, ahead, width // pair)
    columns = pl.ds(first, width)
    some = pl.ds(piece * step, step)
    copies = [
        pltpu.make_async_copy(gain_ref.at[:, columns], gains, sems.at[0]),
        pltpu.make_async_copy(hidden_ref.at[some, columns], rows, sems.at[1]),
    ]
    for copy in copies:
        copy.start()
    for copy in copies:
        copy.wait()
    put_scaled(out_ref, rows, gains, slice(None), core)


def away(hidden, gain, parts, pair, held, ahead, piece):
    step, width = hidden.shape[0] // PIECES, pair * held
    return pl.pallas_call(
        functools.partial(away_kernel, parts, pair, ahead, piece),
        in_specs=[HBM, HBM],
        out_specs=VMEM,
        out_shape=jax.ShapeDtypeStruct((step, width), jnp.bfloat16),
        scratch_shapes=[
            pltpu.VMEM((step, width), jnp.bfloat16),
            pltpu.VMEM((1, width), jnp.float32),
            pltpu.SemaphoreType.DMA((2,)),
        ],
        compiler_params=pltpu.CompilerParams(vmem_limit_bytes=8 * MIB),
        name="away",
    )(in_hbm(hidden), in_hbm(gain))


def home_kernel(parts, pair, hidden_ref, gain_ref, weight_ref, *refs):
    out_ref, power_ref, held_ref, rows, gains, sems = refs
    copies = [
        pltpu.make_async_copy(gain_ref, gains, sems.at[0]),
        pltpu.make_async_copy(hidden_ref, rows, sems.at[1]),
        pltpu.make_async_copy(weight_ref, held_ref, sems.at[2]),
    ]
    for copy in copies:
        copy.start()
    for copy in copies[:2]:
        copy.wait()
    width = out_ref.shape[1]
    first, core = place_of(parts, pair, 0, width // pair)
    columns = pl.ds(first, width)
    put_scaled(out_ref, rows.at[:, columns], gains.at[:, columns], slice(None), core)
    tokens, model = rows.shape
    total = jnp.zeros((tokens, HD), jnp.float32)
    for j in range(0, model, HD):
        wide = rows[:, j : j + HD].astype(jnp.float32)
        total += wide * wide
    mean = jnp.sum(total, axis=1, keepdims=True) / model
    power_ref[...] = lax.rsqrt(mean + EPS)
    copies[2].wait()


def home(hidden, gain, weight, parts, pair):
    tokens, model = hidden.shape
    return pl.pallas_call(
        functools.partial(home_kernel, parts, pair),
        in_specs=[HBM] * 3,
        out_specs=[VMEM] * 3,
        out_shape=[
            jax.ShapeDtypeStruct((tokens, pair * weight.shape[0]), jnp.bfloat16),
            jax.ShapeDtypeStruct((tokens, 1), jnp.float32),
            jax.ShapeDtypeStruct(weight.shape, weight.dtype),
        ],
        scratch_shapes=[
            pltpu.VMEM((tokens, model), jnp.bfloat16),
            pltpu.VMEM((1, model), jnp.float32),
            pltpu.SemaphoreType.DMA((3,)),
        ],
        compiler_params=pltpu.CompilerParams(vmem_limit_bytes=16 * MIB),
        name="home",
    )(in_hbm(hidden), in_hbm(gain), in_hbm(weight))


def columns_of(chunks):
    return [
        (half * KVH * HD + heads[0] * HD, len(heads) * HD) for heads in chunks for half in range(2)
    ]


def project_kernel(runs, skip, counts, *refs):
    ready, rows = refs[: counts[0]], refs[counts[0] : sum(counts[:2])]
    weights, out_ref = refs[sum(counts[:2]) : -1], refs[-1]
    depth = weights[0].shape[0]
    row = 0
    for ready_ref in ready:
        row = ready_ref.shape[0]
        out_ref[:row, :] = ready_ref[:, skip : skip + out_ref.shape[1]]
    for rows_ref in rows:
        some = slice(row, row + rows_ref.shape[0])
        row = some.stop
        column = 0
        for start, width in runs:
            total = None
            for w, weight in enumerate(weights):
                term = jnp.dot(
                    rows_ref[:, w * depth : (w + 1) * depth],
                    weight[:, start : start + width],
                    preferred_element_type=jnp.float32,
                )
                total = term if total is None else total + term
            out_ref[some, column : column + width] = total.astype(out_ref.dtype)
            column += width


def project(rows, weights, chunks, dtype, ready=(), skip=0):
    tokens = sum(r.shape[0] for r in (*ready, *rows))
    depth = rows[0].shape[1]
    runs = columns_of(chunks)
    columns = sum(width for _, width in runs)
    operands = [*ready, *rows, *weights]
    return pl.pallas_call(
        functools.partial(project_kernel, runs, skip, (len(ready), len(rows))),
        in_specs=[VMEM] * len(operands),
        out_specs=VMEM,
        out_shape=jax.ShapeDtypeStruct((tokens, columns), dtype),
        compiler_params=pltpu.CompilerParams(vmem_limit_bytes=24 * MIB),
        cost_estimate=pl.CostEstimate(
            flops=2 * rows[0].shape[0] * len(rows) * depth * columns,
            bytes_accessed=2 * depth * columns,
            transcendentals=0,
        ),
        name="project",
    )(*operands)


def merge_kernel(heads, own, other, pieces, mine_ref, power_ref, bias_ref, *refs):
    parts, out_ref = refs[:-1], refs[-1]
    width = len(heads) * HD
    step = out_ref.shape[0] // pieces
    for piece in range(pieces):
        some = slice(piece * step, (piece + 1) * step)
        power = power_ref[some, :]
        for half in range(2):
            total = mine_ref[some, own[half] : own[half] + width]
            for part in parts[piece::pieces]:
                total = total + part[:, other[half] : other[half] + width].astype(jnp.float32)
            if half == 0:
                total = total * (power * (HD ** (-0.5) * LOG2E))
            else:
                first = heads[0] * HD
                total = total * power + bias_ref[:, first : first + width]
            out_ref[some, half * width : (half + 1) * width] = total.astype(jnp.bfloat16)


def merge(mine, power, bias, parts, pieces, heads, own, other):
    return pl.pallas_call(
        functools.partial(merge_kernel, heads, own, other, pieces),
        in_specs=[VMEM] * (3 + len(parts)),
        out_specs=VMEM,
        out_shape=jax.ShapeDtypeStruct((mine.shape[0], 2 * len(heads) * HD), jnp.bfloat16),
        compiler_params=pltpu.CompilerParams(vmem_limit_bytes=4 * MIB),
        name="merge",
    )(mine, power, bias, *parts)


def pick_kernel(even_ref, odd_ref, out_ref):
    odd = lax.rem(lax.axis_index("sp"), jnp.int32(2)) == 1

    @pl.when(odd)
    def _():
        out_ref[...] = odd_ref[...]

    @pl.when(jnp.logical_not(odd))
    def _():
        out_ref[...] = even_ref[...]


def pick(even, odd):
    return pl.pallas_call(
        pick_kernel,
        in_specs=[VMEM] * 2,
        out_specs=VMEM,
        out_shape=jax.ShapeDtypeStruct(even.shape, even.dtype),
        compiler_params=pltpu.CompilerParams(vmem_limit_bytes=4 * MIB),
        name="pick",
    )(even, odd)


def mask_kernel(reach, lengths_ref, out_ref):
    tokens, window = out_ref.shape
    first = lax.axis_index("sp") * tokens
    query_pos = first + lax.broadcasted_iota(jnp.int32, (tokens, HD), 0)
    start = jnp.zeros((tokens, HD), jnp.int32)
    end = jnp.int32(0)
    for i in range(lengths_ref.shape[1]):
        end = end + lengths_ref[0, i]
        start = jnp.where(query_pos >= end, end, start)
    for j in range(0, window, HD):
        key_pos = first - reach * tokens + j + lax.broadcasted_iota(jnp.int32, (tokens, HD), 1)
        allowed = (key_pos >= start) & (key_pos <= query_pos)
        out_ref[:, j : j + HD] = jnp.where(allowed, 0.0, MASKED).astype(jnp.float32)


def mask(lengths, tokens, reach):
    return pl.pallas_call(
        functools.partial(mask_kernel, reach),
        in_specs=[SMEM],
        out_specs=VMEM,
        out_shape=jax.ShapeDtypeStruct((tokens, (reach + 1) * tokens), jnp.float32),
        compiler_params=pltpu.CompilerParams(vmem_limit_bytes=4 * MIB),
        name="mask",
    )(lengths)


def attend_kernel(count, first, bias_ref, query_ref, *refs):
    blocks, (out_ref, scores, probs, tiles, sems) = refs[:count], refs[-5:]
    tokens = query_ref.shape[0]
    heads = blocks[0].shape[1] // (2 * HD)
    span = scores.shape[2]
    buffers = scores.shape[0]
    units = [(head, t) for head in range(heads) for t in range(0, tokens, TILE)]

    def spans(t):
        for b in range(count):
            a, z = max(t - b * tokens, 0), min(t + span - b * tokens, tokens)
            if a < z:
                yield b, a, z, b * tokens + a - t

    def score(u):
        head, t = units[u]
        wide = (first + head) * RATIO * HD
        queries = [
            query_ref[t : t + TILE, wide + h * HD : wide + (h + 1) * HD] for h in range(RATIO)
        ]
        queries = jnp.concatenate(queries, axis=0)
        for b, a, z, at in spans(t):
            scores[u % buffers, :, at : at + z - a] = lax.dot_general(
                queries,
                blocks[b][a:z, head * HD : (head + 1) * HD],
                (((1,), (1,)), ((), ())),
                preferred_element_type=jnp.float32,
            )

    def soften(u):
        t = units[u][1]
        for r in range(0, RATIO * TILE, STRIP):
            m = t + r % TILE
            some = scores[u % buffers, r : r + STRIP, :] + bias_ref[m : m + STRIP, t : t + span]
            highest = jnp.max(some, axis=1, keepdims=True)
            probs[u % buffers, r : r + STRIP, :] = jnp.exp2(some - highest).astype(jnp.bfloat16)

    def blend(u):
        head, t = units[u]
        total = None
        for b, a, z, at in spans(t):
            value = blocks[b][a:z, (heads + head) * HD : (heads + head + 1) * HD]
            value = jnp.concatenate([value, jnp.ones((z - a, HD), jnp.bfloat16)], axis=1)
            term = jnp.dot(
                probs[u % buffers, :, at : at + z - a], value, preferred_element_type=jnp.float32
            )
            total = term if total is None else total + term
        result = (total[:, :HD] / total[:, HD:]).astype(out_ref.dtype)
        for h in range(RATIO):
            tiles[u, :, h * HD : (h + 1) * HD] = result[h * TILE : (h + 1) * TILE]
        wide = (first + head) * RATIO * HD
        place = out_ref.at[t : t + TILE, wide : wide + RATIO * HD]
        copy = pltpu.make_async_copy(tiles.at[u], place, sems.at[u])
        copy.start()
        return copy

    for u in range(min(AHEAD, len(units))):
        score(u)
    copies = []
    for u in range(len(units)):
        if u + AHEAD < len(units):
            score(u + AHEAD)
        soften(u)
        copies.append(blend(u))
    for copy in copies:
        copy.wait()


def attend(bias, queries, blocks, heads, partial):
    tokens = queries.shape[0]
    in_specs = [VMEM] * (2 + len(blocks))
    operands = [bias, queries, *blocks]
    aliases = {}
    if partial is not None:
        aliases = {len(operands): 0}
        operands.append(in_hbm(partial))
        in_specs.append(HBM)
    span = (len(blocks) - 1) * tokens + TILE
    units = len(heads) * tokens // TILE
    return pl.pallas_call(
        functools.partial(attend_kernel, len(blocks), heads[0]),
        in_specs=in_specs,
        out_specs=HBM,
        out_shape=pltpu.HBM((tokens, QH * HD), jnp.bfloat16),
        scratch_shapes=[
            pltpu.VMEM((AHEAD + 1, RATIO * TILE, span), jnp.float32),
            pltpu.VMEM((AHEAD + 1, RATIO * TILE, span), jnp.bfloat16),
            pltpu.VMEM((units, TILE, RATIO * HD), jnp.bfloat16),
            pltpu.SemaphoreType.DMA((units,)),
        ],
        input_output_aliases=aliases,
        compiler_params=pltpu.CompilerParams(vmem_limit_bytes=24 * MIB),
        cost_estimate=pl.CostEstimate(
            flops=6 * tokens * len(heads) * RATIO * HD * span,
            bytes_accessed=4 * tokens * len(heads) * RATIO * HD,
            transcendentals=len(heads) * RATIO * tokens * span,
        ),
        name="attend",
    )(*operands)


def shards(hidden, queries, norm_gain, kv_weight, value_bias, doc_lengths):
    return layer(hidden[0], queries[0], norm_gain, kv_weight, value_bias, doc_lengths)[None]


def layer(hidden, queries, norm_gain, kv_weight, value_bias, doc_lengths):
    tokens = hidden.shape[0]
    parts = lax.axis_size("fsdp")
    length = lax.axis_size("sp")
    held = kv_weight.shape[0]
    pair = 2 if parts % 2 == 0 else 1
    groups = parts // pair
    reach = length // 4
    gain = norm_gain[None]

    arrived = []
    for d in range(1, groups):
        there = [(i, (i + d * pair) % parts) for i in range(parts)]
        arrived.append([])
        for p in range(PIECES):
            sent = away(hidden, gain, parts, pair, held, d, p)
            arrived[-1].append(lax.ppermute(sent, "fsdp", there))
    own, power, kept = home(hidden, gain, kv_weight, parts, pair)
    weights = [kept]
    if pair == 2:
        weights.append(lax.ppermute(kv_weight, "fsdp", [(i, i ^ 1) for i in range(parts)]))
    bias = mask(doc_lengths, tokens, reach)
    mine = project([own], weights, SUMS, jnp.float32)

    early = []
    for d in range(1, groups):
        early.append(project(arrived[d - 1][:1], weights, SUMS[1:], jnp.bfloat16))

    returned = []
    skip = 0
    for c, heads in enumerate(SUMS):
        returned.append([])
        for d in range(1, groups):
            back = [(i, (i - d * pair) % parts) for i in range(parts)]
            for p in range(PIECES if c == 0 else 1):
                if c == 0:
                    part = project(arrived[d - 1][p : p + 1], weights, [heads], jnp.bfloat16)
                else:
                    rows, ready = arrived[d - 1][1:], early[d - 1 : d]
                    part = project(rows, weights, [heads], jnp.bfloat16, ready, skip)
                returned[-1].append(lax.ppermute(part, "fsdp", back))
        skip += 2 * len(heads) * HD if c else 0

    sums = []
    for heads in BLOCKS:
        source = [i for i, some in enumerate(SUMS) if heads[0] in some][0]
        held_heads = SUMS[source]
        own_start = sum(2 * len(some) * HD for some in SUMS[:source])
        first = (heads[0] - held_heads[0]) * HD
        other_columns = (first, first + len(held_heads) * HD)
        own_columns = tuple(own_start + x for x in other_columns)
        sums.append(
            merge(
                mine,
                power,
                value_bias[None],
                returned[source],
                PIECES if source == 0 else 1,
                heads,
                own_columns,
                other_columns,
            )
        )

    out = None
    for c, heads in enumerate(BLOCKS):
        chain = [sums[c]]
        shifts = range(1, reach + 1)
        swaps = reach % 2 == 0 and length % 2 == 0
        if swaps:
            shifts = range(2, reach + 1, 2)
        for b in shifts:
            ahead = [(i, (i + b) % length) for i in range(length)]
            chain.append(lax.ppermute(sums[c], "sp", ahead))
        blocks = chain
        if swaps:
            blocks = [chain[0]]
            swap = [(i, i ^ 1) for i in range(length)]
            for b in range(reach // 2):
                near = lax.ppermute(pick(chain[b], chain[b + 1]), "sp", swap)
                blocks += [near, chain[b + 1]]
        out = attend(bias, queries, blocks[::-1], heads, out)
    return out


def solution(mesh):
    in_specs = (
        P("fsdp", "sp", None),
        P("fsdp", "sp", None),
        P(),
        P("fsdp", None),
        P(),
        P("fsdp", None),
    )
    out_specs = P("fsdp", "sp", None)
    return jax.shard_map(shards, mesh=mesh, in_specs=in_specs, out_specs=out_specs, check_vma=False)
```

```python
import functools

import jax
import jax.numpy as jnp
from jax import lax
from jax.experimental import pallas as pl
from jax.experimental.pallas import tpu as pltpu
from jax.sharding import PartitionSpec as P

QH = 32
KVH = 8
HD = 128
EPS = 1e-06
RATIO = QH // KVH
LOG2E = 1.4426950408889634
SUMS = ((0, 1), (2, 3), (4, 5), (6, 7))
BLOCKS = ((0, 1), (2, 3), (4, 5), (6,), (7,))
PIECES = 2
FIRST = 3, 4
TILE = 128
STRIP = 32
AHEAD = 2
MASKED = -1e30
MIB = 1 << 20
VMEM = pl.BlockSpec(memory_space=pltpu.VMEM)
SMEM = pl.BlockSpec(memory_space=pltpu.SMEM)
HBM = pl.BlockSpec(memory_space=pltpu.HBM)


def across(place, ahead, parts, pair):
    group, core = divmod(place, pair)
    return (group + ahead) % (parts // pair) * pair + (pair - 1 - core)


def in_hbm(value):
    return pltpu.with_memory_space_constraint(value, pltpu.HBM)


def place_of(parts, pair, ahead, held):
    me = lax.axis_index("fsdp")
    group, core = lax.div(me, jnp.int32(pair)), lax.rem(me, jnp.int32(pair))
    there = lax.rem(group + ahead, jnp.int32(parts // pair))
    return pl.multiple_of(there * (pair * held), HD), core


def put_scaled(out_ref, rows_ref, gain_ref, some, core):
    held = out_ref.shape[1] // 2

    @pl.when(core == 0)
    def _():
        out_ref[...] = (rows_ref[some, :].astype(jnp.float32) * gain_ref[...]).astype(jnp.bfloat16)

    @pl.when(core == 1)
    def _():
        for a, b in ((0, held), (held, 0)):
            wide = rows_ref[some, a : a + held].astype(jnp.float32)
            scaled = wide * gain_ref[:, a : a + held]
            out_ref[:, b : b + held] = scaled.astype(jnp.bfloat16)


def bounds_of(tokens):
    cut = tokens * FIRST[0] // FIRST[1]
    return (0, cut, tokens)


def away_kernel(parts, pair, ahead, start, hidden_ref, gain_ref, out_ref, rows, gains, sems):
    step, width = rows.shape
    first, core = place_of(parts, pair, ahead, width // pair)
    columns = pl.ds(first, width)
    some = pl.ds(start, step)
    copies = [
        pltpu.make_async_copy(gain_ref.at[:, columns], gains, sems.at[0]),
        pltpu.make_async_copy(hidden_ref.at[some, columns], rows, sems.at[1]),
    ]
    for copy in copies:
        copy.start()
    for copy in copies:
        copy.wait()
    put_scaled(out_ref, rows, gains, slice(None), pair - 1 - core)


def away(hidden, gain, parts, pair, held, ahead, piece):
    start, stop = bounds_of(hidden.shape[0])[piece : piece + 2]
    step, width = stop - start, pair * held
    return pl.pallas_call(
        functools.partial(away_kernel, parts, pair, ahead, start),
        in_specs=[HBM, HBM],
        out_specs=VMEM,
        out_shape=pltpu.VMEM((step, width), jnp.bfloat16),
        scratch_shapes=[
            pltpu.VMEM((step, width), jnp.bfloat16),
            pltpu.VMEM((1, width), jnp.float32),
            pltpu.SemaphoreType.DMA((2,)),
        ],
        compiler_params=pltpu.CompilerParams(vmem_limit_bytes=58 * MIB),
        name="away",
    )(in_hbm(hidden), in_hbm(gain))


def home_kernel(parts, pair, hidden_ref, gain_ref, weight_ref, *refs):
    out_ref, power_ref, held_ref, rows, gains, sems = refs
    copies = [
        pltpu.make_async_copy(gain_ref, gains, sems.at[0]),
        pltpu.make_async_copy(hidden_ref, rows, sems.at[1]),
        pltpu.make_async_copy(weight_ref, held_ref, sems.at[2]),
    ]
    for copy in copies:
        copy.start()
    for copy in copies[:2]:
        copy.wait()
    width = out_ref.shape[1]
    first, core = place_of(parts, pair, 0, width // pair)
    columns = pl.ds(first, width)
    put_scaled(out_ref, rows.at[:, columns], gains.at[:, columns], slice(None), core)
    tokens, model = rows.shape
    total = jnp.zeros((tokens, HD), jnp.float32)
    for j in range(0, model, HD):
        wide = rows[:, j : j + HD].astype(jnp.float32)
        total += wide * wide
    mean = jnp.sum(total, axis=1, keepdims=True) / model
    power_ref[...] = lax.rsqrt(mean + EPS)
    copies[2].wait()


def home(hidden, gain, weight, parts, pair):
    tokens, model = hidden.shape
    return pl.pallas_call(
        functools.partial(home_kernel, parts, pair),
        in_specs=[HBM] * 3,
        out_specs=[VMEM] * 3,
        out_shape=[
            jax.ShapeDtypeStruct((tokens, pair * weight.shape[0]), jnp.bfloat16),
            jax.ShapeDtypeStruct((tokens, 1), jnp.float32),
            jax.ShapeDtypeStruct(weight.shape, weight.dtype),
        ],
        scratch_shapes=[
            pltpu.VMEM((tokens, model), jnp.bfloat16),
            pltpu.VMEM((1, model), jnp.float32),
            pltpu.SemaphoreType.DMA((3,)),
        ],
        compiler_params=pltpu.CompilerParams(vmem_limit_bytes=16 * MIB),
        name="home",
    )(in_hbm(hidden), in_hbm(gain), in_hbm(weight))


def columns_of(chunks):
    return [
        (half * KVH * HD + heads[0] * HD, len(heads) * HD) for heads in chunks for half in range(2)
    ]


def project_kernel(runs, skip, counts, *refs):
    ready, rows = refs[: counts[0]], refs[counts[0] : sum(counts[:2])]
    weights, out_ref = refs[sum(counts[:2]) : -1], refs[-1]
    depth = weights[0].shape[0]
    row = 0
    for ready_ref in ready:
        row = ready_ref.shape[0]
        out_ref[:row, :] = ready_ref[:, skip : skip + out_ref.shape[1]]
    for rows_ref in rows:
        some = slice(row, row + rows_ref.shape[0])
        row = some.stop
        column = 0
        for start, width in runs:
            total = None
            for w, weight in enumerate(weights):
                term = jnp.dot(
                    rows_ref[:, w * depth : (w + 1) * depth],
                    weight[:, start : start + width],
                    preferred_element_type=jnp.float32,
                )
                total = term if total is None else total + term
            out_ref[some, column : column + width] = total.astype(out_ref.dtype)
            column += width


def project(rows, weights, chunks, dtype, ready=(), skip=0):
    tokens = sum(r.shape[0] for r in (*ready, *rows))
    depth = rows[0].shape[1]
    runs = columns_of(chunks)
    columns = sum(width for _, width in runs)
    operands = [*ready, *rows, *weights]
    return pl.pallas_call(
        functools.partial(project_kernel, runs, skip, (len(ready), len(rows))),
        in_specs=[VMEM] * len(operands),
        out_specs=VMEM,
        out_shape=jax.ShapeDtypeStruct((tokens, columns), dtype),
        compiler_params=pltpu.CompilerParams(vmem_limit_bytes=24 * MIB),
        cost_estimate=pl.CostEstimate(
            flops=2 * rows[0].shape[0] * len(rows) * depth * columns,
            bytes_accessed=2 * depth * columns,
            transcendentals=0,
        ),
        name="project",
    )(*operands)


def merge_kernel(heads, own, other, pieces, mine_ref, power_ref, bias_ref, *refs):
    parts, out_ref = refs[:-1], refs[-1]
    width = len(heads) * HD
    bounds = bounds_of(out_ref.shape[0]) if pieces > 1 else (0, out_ref.shape[0])
    for piece in range(pieces):
        some = slice(bounds[piece], bounds[piece + 1])
        power = power_ref[some, :]
        for half in range(2):
            total = mine_ref[some, own[half] : own[half] + width]
            for part in parts[piece::pieces]:
                total = total + part[:, other[half] : other[half] + width].astype(jnp.float32)
            if half == 0:
                total = total * (power * (HD ** (-0.5) * LOG2E))
            else:
                first = heads[0] * HD
                total = total * power + bias_ref[:, first : first + width]
            out_ref[some, half * width : (half + 1) * width] = total.astype(jnp.bfloat16)


def merge(mine, power, bias, parts, pieces, heads, own, other):
    return pl.pallas_call(
        functools.partial(merge_kernel, heads, own, other, pieces),
        in_specs=[VMEM] * (3 + len(parts)),
        out_specs=VMEM,
        out_shape=jax.ShapeDtypeStruct((mine.shape[0], 2 * len(heads) * HD), jnp.bfloat16),
        compiler_params=pltpu.CompilerParams(vmem_limit_bytes=4 * MIB),
        name="merge",
    )(mine, power, bias, *parts)


def pick_kernel(even_ref, odd_ref, out_ref):
    odd = lax.rem(lax.axis_index("sp"), jnp.int32(2)) == 1

    @pl.when(odd)
    def _():
        out_ref[...] = odd_ref[...]

    @pl.when(jnp.logical_not(odd))
    def _():
        out_ref[...] = even_ref[...]


def pick(even, odd):
    return pl.pallas_call(
        pick_kernel,
        in_specs=[VMEM] * 2,
        out_specs=VMEM,
        out_shape=jax.ShapeDtypeStruct(even.shape, even.dtype),
        compiler_params=pltpu.CompilerParams(vmem_limit_bytes=4 * MIB),
        name="pick",
    )(even, odd)


def mask_kernel(reach, lengths_ref, out_ref):
    tokens, window = out_ref.shape
    first = lax.axis_index("sp") * tokens
    query_pos = first + lax.broadcasted_iota(jnp.int32, (tokens, HD), 0)
    start = jnp.zeros((tokens, HD), jnp.int32)
    end = jnp.int32(0)
    for i in range(lengths_ref.shape[1]):
        end = end + lengths_ref[0, i]
        start = jnp.where(query_pos >= end, end, start)
    for j in range(0, window, HD):
        key_pos = first - reach * tokens + j + lax.broadcasted_iota(jnp.int32, (tokens, HD), 1)
        allowed = (key_pos >= start) & (key_pos <= query_pos)
        out_ref[:, j : j + HD] = jnp.where(allowed, 0.0, MASKED).astype(jnp.float32)


def mask(lengths, tokens, reach):
    return pl.pallas_call(
        functools.partial(mask_kernel, reach),
        in_specs=[SMEM],
        out_specs=VMEM,
        out_shape=jax.ShapeDtypeStruct((tokens, (reach + 1) * tokens), jnp.float32),
        compiler_params=pltpu.CompilerParams(vmem_limit_bytes=4 * MIB),
        name="mask",
    )(lengths)


def flush(tiles, out_ref, sems, first):
    per_head = out_ref.shape[0] // TILE
    copies = []
    for u in range(tiles.shape[0]):
        t = u % per_head * TILE
        wide = (first + u // per_head) * RATIO * HD
        place = out_ref.at[t : t + TILE, wide : wide + RATIO * HD]
        copies.append(pltpu.make_async_copy(tiles.at[u], place, sems.at[u]))
    return copies


def attend_kernel(count, first, before, aliased, last, bias_ref, query_ref, *refs):
    blocks, refs = refs[:count], list(refs[count:])
    out_ref, copies = None, []
    if before is not None:
        older = refs.pop(0)
        if aliased:
            refs.pop(0)
        out_ref = refs.pop(0)
        copies = flush(older, out_ref, refs[-1], before)
        for copy in copies:
            copy.start()
    tiles, scores, probs = refs[:3]
    tokens = query_ref.shape[0]
    heads = blocks[0].shape[1] // (2 * HD)
    span = scores.shape[2]
    buffers = scores.shape[0]
    units = [(head, t) for head in range(heads) for t in range(0, tokens, TILE)]

    def spans(t):
        for b in range(count):
            a, z = max(t - b * tokens, 0), min(t + span - b * tokens, tokens)
            if a < z:
                yield b, a, z, b * tokens + a - t

    def score(u):
        head, t = units[u]
        wide = (first + head) * RATIO * HD
        queries = [
            query_ref[t : t + TILE, wide + h * HD : wide + (h + 1) * HD] for h in range(RATIO)
        ]
        queries = jnp.concatenate(queries, axis=0)
        for b, a, z, at in spans(t):
            scores[u % buffers, :, at : at + z - a] = lax.dot_general(
                queries,
                blocks[b][a:z, head * HD : (head + 1) * HD],
                (((1,), (1,)), ((), ())),
                preferred_element_type=jnp.float32,
            )

    def soften(u):
        t = units[u][1]
        for r in range(0, RATIO * TILE, STRIP):
            m = t + r % TILE
            some = scores[u % buffers, r : r + STRIP, :] + bias_ref[m : m + STRIP, t : t + span]
            highest = jnp.max(some, axis=1, keepdims=True)
            probs[u % buffers, r : r + STRIP, :] = jnp.exp2(some - highest).astype(jnp.bfloat16)

    def blend(u):
        head, t = units[u]
        total = None
        for b, a, z, at in spans(t):
            value = blocks[b][a:z, (heads + head) * HD : (heads + head + 1) * HD]
            value = jnp.concatenate([value, jnp.ones((z - a, HD), jnp.bfloat16)], axis=1)
            term = jnp.dot(
                probs[u % buffers, :, at : at + z - a], value, preferred_element_type=jnp.float32
            )
            total = term if total is None else total + term
        result = (total[:, :HD] / total[:, HD:]).astype(tiles.dtype)
        for h in range(RATIO):
            tiles[u, :, h * HD : (h + 1) * HD] = result[h * TILE : (h + 1) * TILE]

    ours = flush(tiles, out_ref, refs[3], first) if last else []
    for u in range(min(AHEAD, len(units))):
        score(u)
    for u in range(len(units)):
        if u + AHEAD < len(units):
            score(u + AHEAD)
        soften(u)
        blend(u)
        if last:
            ours[u].start()
    for copy in copies + ours:
        copy.wait()


def attend(bias, queries, blocks, heads, before, last):
    tokens = queries.shape[0]
    operands = [bias, queries, *blocks]
    in_specs = [VMEM] * len(operands)
    span = (len(blocks) - 1) * tokens + TILE
    units = len(heads) * tokens // TILE
    tile = (TILE, RATIO * HD)
    aliases = {}
    out_specs, out_shape, scratch = [], [], []
    older_heads = None
    older_units = 0
    if before is not None:
        older_heads, older, partial = before
        older_units = older.shape[0]
        operands.append(older)
        in_specs.append(VMEM)
        if partial is not None:
            aliases = {len(operands): 0}
            operands.append(in_hbm(partial))
            in_specs.append(HBM)
        out_specs.append(HBM)
        out_shape.append(pltpu.HBM((tokens, QH * HD), jnp.bfloat16))
    if last:
        scratch.append(pltpu.VMEM((units, *tile), jnp.bfloat16))
    else:
        out_specs.append(VMEM)
        out_shape.append(pltpu.VMEM((units, *tile), jnp.bfloat16))
    scratch += [
        pltpu.VMEM((AHEAD + 1, RATIO * TILE, span), jnp.float32),
        pltpu.VMEM((AHEAD + 1, RATIO * TILE, span), jnp.bfloat16),
    ]
    if last:
        scratch.append(pltpu.SemaphoreType.DMA((units,)))
    if before is not None:
        scratch.append(pltpu.SemaphoreType.DMA((older_units,)))
    return pl.pallas_call(
        functools.partial(
            attend_kernel,
            len(blocks),
            heads[0],
            None if before is None else older_heads[0],
            bool(aliases),
            last,
        ),
        in_specs=in_specs,
        out_specs=out_specs,
        out_shape=out_shape,
        scratch_shapes=scratch,
        input_output_aliases=aliases,
        compiler_params=pltpu.CompilerParams(vmem_limit_bytes=24 * MIB),
        cost_estimate=pl.CostEstimate(
            flops=6 * tokens * len(heads) * RATIO * HD * span,
            bytes_accessed=4 * tokens * len(heads) * RATIO * HD,
            transcendentals=len(heads) * RATIO * tokens * span,
        ),
        name="attend",
    )(*operands)


def shards(hidden, queries, norm_gain, kv_weight, value_bias, doc_lengths):
    return layer(hidden[0], queries[0], norm_gain, kv_weight, value_bias, doc_lengths)[None]


def layer(hidden, queries, norm_gain, kv_weight, value_bias, doc_lengths):
    tokens = hidden.shape[0]
    parts = lax.axis_size("fsdp")
    length = lax.axis_size("sp")
    held = kv_weight.shape[0]
    pair = 2 if parts % 2 == 0 else 1
    groups = parts // pair
    reach = length // 4
    gain = norm_gain[None]

    arrived = []
    for d in range(1, groups):
        there = [(i, across(i, d, parts, pair)) for i in range(parts)]
        arrived.append([])
        for p in range(PIECES):
            sent = away(hidden, gain, parts, pair, held, d, p)
            arrived[-1].append(lax.ppermute(sent, "fsdp", there))
    own, power, kept = home(hidden, gain, kv_weight, parts, pair)
    weights = [kept]
    if pair == 2:
        weights.append(lax.ppermute(kv_weight, "fsdp", [(i, i ^ 1) for i in range(parts)]))
    bias = mask(doc_lengths, tokens, reach)
    mine = project([own], weights, SUMS, jnp.float32)

    early = []
    for d in range(1, groups):
        early.append(project(arrived[d - 1][:1], weights, SUMS[1:], jnp.bfloat16))

    returned = []
    skip = 0
    for c, heads in enumerate(SUMS):
        returned.append([])
        for d in range(1, groups):
            back = [(across(i, d, parts, pair), i) for i in range(parts)]
            for p in range(PIECES if c == 0 else 1):
                if c == 0:
                    part = project(arrived[d - 1][p : p + 1], weights, [heads], jnp.bfloat16)
                else:
                    rows, ready = arrived[d - 1][1:], early[d - 1 : d]
                    part = project(rows, weights, [heads], jnp.bfloat16, ready, skip)
                returned[-1].append(lax.ppermute(part, "fsdp", back))
        skip += 2 * len(heads) * HD if c else 0

    sums = []
    for heads in BLOCKS:
        source = [i for i, some in enumerate(SUMS) if heads[0] in some][0]
        held_heads = SUMS[source]
        own_start = sum(2 * len(some) * HD for some in SUMS[:source])
        first = (heads[0] - held_heads[0]) * HD
        other_columns = (first, first + len(held_heads) * HD)
        own_columns = tuple(own_start + x for x in other_columns)
        sums.append(
            merge(
                mine,
                power,
                value_bias[None],
                returned[source],
                PIECES if source == 0 else 1,
                heads,
                own_columns,
                other_columns,
            )
        )

    before = None
    for c, heads in enumerate(BLOCKS):
        chain = [sums[c]]
        shifts = range(1, reach + 1)
        swaps = reach % 2 == 0 and length % 2 == 0
        if swaps:
            shifts = range(2, reach + 1, 2)
        for b in shifts:
            ahead = [(i, (i + b) % length) for i in range(length)]
            chain.append(lax.ppermute(sums[c], "sp", ahead))
        blocks = chain
        if swaps:
            blocks = [chain[0]]
            swap = [(i, i ^ 1) for i in range(length)]
            for b in range(reach // 2):
                near = lax.ppermute(pick(chain[b], chain[b + 1]), "sp", swap)
                blocks += [near, chain[b + 1]]
        last = c == len(BLOCKS) - 1
        results = attend(bias, queries, blocks[::-1], heads, before, last)
        before = (heads, results[-1], results[0] if before is not None else None)
    return results[0]


def solution(mesh):
    in_specs = (
        P("fsdp", "sp", None),
        P("fsdp", "sp", None),
        P(),
        P("fsdp", None),
        P(),
        P("fsdp", None),
    )
    out_specs = P("fsdp", "sp", None)
    return jax.shard_map(shards, mesh=mesh, in_specs=in_specs, out_specs=out_specs, check_vma=False)
```

```python
import functools

import jax
import jax.numpy as jnp
from jax import lax
from jax.experimental import pallas as pl
from jax.experimental.pallas import tpu as pltpu
from jax.sharding import PartitionSpec as P

QH = 32
KVH = 8
HD = 128
EPS = 1e-06
RATIO = QH // KVH
LOG2E = 1.4426950408889634
GROUPS = ((0, 1, 2), (3, 4, 5), (6, 7))
CHUNKS = ((0, 0), (0, 1), (1, 0), (1, 1), (0, 2), (1, 2))
PIECES = 2
TILE = 128
STRIP = 32
AHEAD = 2
MASKED = -1e30
MIB = 1 << 20
VMEM = pl.BlockSpec(memory_space=pltpu.VMEM)
SMEM = pl.BlockSpec(memory_space=pltpu.SMEM)
HBM = pl.BlockSpec(memory_space=pltpu.HBM)


def across(place, ahead, parts, pair):
    group, core = divmod(place, pair)
    return (group + ahead) % (parts // pair) * pair + (pair - 1 - core)


def in_hbm(value):
    return pltpu.with_memory_space_constraint(value, pltpu.HBM)


def place_of(parts, pair, ahead, held):
    me = lax.axis_index("fsdp")
    group, core = lax.div(me, jnp.int32(pair)), lax.rem(me, jnp.int32(pair))
    there = lax.rem(group + ahead, jnp.int32(parts // pair))
    return pl.multiple_of(there * (pair * held), HD), core


def put_scaled(out_ref, rows_ref, gain_ref, some, core):
    held = out_ref.shape[1] // 2

    @pl.when(core == 0)
    def _():
        out_ref[...] = (rows_ref[some, :].astype(jnp.float32) * gain_ref[...]).astype(jnp.bfloat16)

    @pl.when(core == 1)
    def _():
        for a, b in ((0, held), (held, 0)):
            wide = rows_ref[some, a : a + held].astype(jnp.float32)
            scaled = wide * gain_ref[:, a : a + held]
            out_ref[:, b : b + held] = scaled.astype(jnp.bfloat16)


def away_kernel(parts, pair, ahead, start, hidden_ref, gain_ref, out_ref, rows, gains, sems):
    step, width = rows.shape
    first, core = place_of(parts, pair, ahead, width // pair)
    columns = pl.ds(first, width)
    some = pl.ds(start, step)
    copies = [
        pltpu.make_async_copy(gain_ref.at[:, columns], gains, sems.at[0]),
        pltpu.make_async_copy(hidden_ref.at[some, columns], rows, sems.at[1]),
    ]
    for copy in copies:
        copy.start()
    for copy in copies:
        copy.wait()
    put_scaled(out_ref, rows, gains, slice(None), pair - 1 - core)


def away(hidden, gain, parts, pair, held, ahead, piece):
    step, width = hidden.shape[0] // PIECES, pair * held
    start = piece * step
    return pl.pallas_call(
        functools.partial(away_kernel, parts, pair, ahead, start),
        in_specs=[HBM, HBM],
        out_specs=VMEM,
        out_shape=pltpu.VMEM((step, width), jnp.bfloat16),
        scratch_shapes=[
            pltpu.VMEM((step, width), jnp.bfloat16),
            pltpu.VMEM((1, width), jnp.float32),
            pltpu.SemaphoreType.DMA((2,)),
        ],
        compiler_params=pltpu.CompilerParams(vmem_limit_bytes=58 * MIB),
        name="away",
    )(in_hbm(hidden), in_hbm(gain))


def home_kernel(parts, pair, hidden_ref, gain_ref, weight_ref, *refs):
    out_ref, power_ref, held_ref, rows, gains, sems = refs
    copies = [
        pltpu.make_async_copy(gain_ref, gains, sems.at[0]),
        pltpu.make_async_copy(hidden_ref, rows, sems.at[1]),
        pltpu.make_async_copy(weight_ref, held_ref, sems.at[2]),
    ]
    for copy in copies:
        copy.start()
    for copy in copies[:2]:
        copy.wait()
    width = out_ref.shape[1]
    first, core = place_of(parts, pair, 0, width // pair)
    columns = pl.ds(first, width)
    put_scaled(out_ref, rows.at[:, columns], gains.at[:, columns], slice(None), core)
    tokens, model = rows.shape
    total = jnp.zeros((tokens, HD), jnp.float32)
    for j in range(0, model, HD):
        wide = rows[:, j : j + HD].astype(jnp.float32)
        total += wide * wide
    mean = jnp.sum(total, axis=1, keepdims=True) / model
    power_ref[...] = lax.rsqrt(mean + EPS)
    copies[2].wait()


def home(hidden, gain, weight, parts, pair):
    tokens, model = hidden.shape
    return pl.pallas_call(
        functools.partial(home_kernel, parts, pair),
        in_specs=[HBM] * 3,
        out_specs=[VMEM] * 3,
        out_shape=[
            jax.ShapeDtypeStruct((tokens, pair * weight.shape[0]), jnp.bfloat16),
            jax.ShapeDtypeStruct((tokens, 1), jnp.float32),
            jax.ShapeDtypeStruct(weight.shape, weight.dtype),
        ],
        scratch_shapes=[
            pltpu.VMEM((tokens, model), jnp.bfloat16),
            pltpu.VMEM((1, model), jnp.float32),
            pltpu.SemaphoreType.DMA((3,)),
        ],
        compiler_params=pltpu.CompilerParams(vmem_limit_bytes=16 * MIB),
        name="home",
    )(in_hbm(hidden), in_hbm(gain), in_hbm(weight))


def columns_of(groups):
    return [
        (half * KVH * HD + heads[0] * HD, len(heads) * HD) for heads in groups for half in range(2)
    ]


def project_kernel(runs, rows_ref, *refs):
    weights, out_ref = refs[:-1], refs[-1]
    depth = weights[0].shape[0]
    column = 0
    for start, width in runs:
        total = None
        for w, weight in enumerate(weights):
            term = jnp.dot(
                rows_ref[:, w * depth : (w + 1) * depth],
                weight[:, start : start + width],
                preferred_element_type=jnp.float32,
            )
            total = term if total is None else total + term
        out_ref[:, column : column + width] = total.astype(out_ref.dtype)
        column += width


def project(rows, weights, groups, dtype):
    tokens, depth = rows.shape
    runs = columns_of(groups)
    columns = sum(width for _, width in runs)
    return pl.pallas_call(
        functools.partial(project_kernel, runs),
        in_specs=[VMEM] * (1 + len(weights)),
        out_specs=VMEM,
        out_shape=jax.ShapeDtypeStruct((tokens, columns), dtype),
        compiler_params=pltpu.CompilerParams(vmem_limit_bytes=24 * MIB),
        cost_estimate=pl.CostEstimate(
            flops=2 * tokens * depth * columns,
            bytes_accessed=2 * depth * columns,
            transcendentals=0,
        ),
        name="project",
    )(rows, *weights)


def merge_kernel(row, start, heads, mine_ref, power_ref, bias_ref, *refs):
    parts, out_ref = refs[:-1], refs[-1]
    rows, width = out_ref.shape[0], len(heads) * HD
    some = slice(row, row + rows)
    power = power_ref[some, :]
    for half in range(2):
        ours = slice(half * width, (half + 1) * width)
        total = mine_ref[some, start + half * width : start + (half + 1) * width]
        for part in parts:
            total = total + part[:, ours].astype(jnp.float32)
        if half == 0:
            total = total * (power * (HD ** (-0.5) * LOG2E))
        else:
            total = total * power + bias_ref[:, heads[0] * HD : heads[0] * HD + width]
        out_ref[:, ours] = total.astype(jnp.bfloat16)


def merge(mine, power, bias, parts, row, start, heads):
    return pl.pallas_call(
        functools.partial(merge_kernel, row, start, heads),
        in_specs=[VMEM] * (3 + len(parts)),
        out_specs=VMEM,
        out_shape=jax.ShapeDtypeStruct(parts[0].shape, jnp.bfloat16),
        compiler_params=pltpu.CompilerParams(vmem_limit_bytes=4 * MIB),
        name="merge",
    )(mine, power, bias, *parts)


def pick_kernel(even_ref, odd_ref, out_ref):
    odd = lax.rem(lax.axis_index("sp"), jnp.int32(2)) == 1

    @pl.when(odd)
    def _():
        out_ref[...] = odd_ref[...]

    @pl.when(jnp.logical_not(odd))
    def _():
        out_ref[...] = even_ref[...]


def pick(even, odd):
    return pl.pallas_call(
        pick_kernel,
        in_specs=[VMEM] * 2,
        out_specs=VMEM,
        out_shape=jax.ShapeDtypeStruct(even.shape, even.dtype),
        compiler_params=pltpu.CompilerParams(vmem_limit_bytes=4 * MIB),
        name="pick",
    )(even, odd)


def mask_kernel(reach, lengths_ref, out_ref):
    tokens, window = out_ref.shape
    first = lax.axis_index("sp") * tokens
    query_pos = first + lax.broadcasted_iota(jnp.int32, (tokens, HD), 0)
    start = jnp.zeros((tokens, HD), jnp.int32)
    end = jnp.int32(0)
    for i in range(lengths_ref.shape[1]):
        end = end + lengths_ref[0, i]
        start = jnp.where(query_pos >= end, end, start)
    for j in range(0, window, HD):
        key_pos = first - reach * tokens + j + lax.broadcasted_iota(jnp.int32, (tokens, HD), 1)
        allowed = (key_pos >= start) & (key_pos <= query_pos)
        out_ref[:, j : j + HD] = jnp.where(allowed, 0.0, MASKED).astype(jnp.float32)


def mask(lengths, tokens, reach):
    return pl.pallas_call(
        functools.partial(mask_kernel, reach),
        in_specs=[SMEM],
        out_specs=VMEM,
        out_shape=jax.ShapeDtypeStruct((tokens, (reach + 1) * tokens), jnp.float32),
        compiler_params=pltpu.CompilerParams(vmem_limit_bytes=4 * MIB),
        name="mask",
    )(lengths)


def flush(tiles, out_ref, sems, first):
    per_head = out_ref.shape[0] // TILE
    copies = []
    for u in range(tiles.shape[0]):
        t = u % per_head * TILE
        wide = (first + u // per_head) * RATIO * HD
        place = out_ref.at[t : t + TILE, wide : wide + RATIO * HD]
        copies.append(pltpu.make_async_copy(tiles.at[u], place, sems.at[u]))
    return copies


def attend_kernel(count, first, before, aliased, last, bias_ref, query_ref, *refs):
    blocks, refs = refs[:count], list(refs[count:])
    out_ref, copies = None, []
    if before is not None:
        older = refs.pop(0)
        if aliased:
            refs.pop(0)
        out_ref = refs.pop(0)
        copies = flush(older, out_ref, refs[-1], before)
        for copy in copies:
            copy.start()
    tiles, scores, probs = refs[:3]
    tokens = query_ref.shape[0]
    heads = blocks[0].shape[1] // (2 * HD)
    piece = blocks[0].shape[0]
    span = scores.shape[2]
    buffers = scores.shape[0]
    units = [(head, t) for head in range(heads) for t in range(0, tokens, TILE)]

    def window(t, column):
        picked = []
        for i, block in enumerate(blocks):
            a, z = max(t - i * piece, 0), min(t + span - i * piece, piece)
            if a < z:
                picked.append(block[a:z, column : column + HD])
        return jnp.concatenate(picked, axis=0)

    def score(u):
        head, t = units[u]
        wide = (first + head) * RATIO * HD
        queries = [
            query_ref[t : t + TILE, wide + h * HD : wide + (h + 1) * HD] for h in range(RATIO)
        ]
        scores[u % buffers] = lax.dot_general(
            jnp.concatenate(queries, axis=0),
            window(t, head * HD),
            (((1,), (1,)), ((), ())),
            preferred_element_type=jnp.float32,
        )

    def soften(u):
        t = units[u][1]
        for r in range(0, RATIO * TILE, STRIP):
            m = t + r % TILE
            some = scores[u % buffers, r : r + STRIP, :] + bias_ref[m : m + STRIP, t : t + span]
            highest = jnp.max(some, axis=1, keepdims=True)
            probs[u % buffers, r : r + STRIP, :] = jnp.exp2(some - highest).astype(jnp.bfloat16)

    def blend(u):
        head, t = units[u]
        values = window(t, (heads + head) * HD)
        values = jnp.concatenate([values, jnp.ones_like(values)], axis=1)
        total = jnp.dot(probs[u % buffers], values, preferred_element_type=jnp.float32)
        result = (total[:, :HD] / total[:, HD:]).astype(tiles.dtype)
        for h in range(RATIO):
            tiles[u, :, h * HD : (h + 1) * HD] = result[h * TILE : (h + 1) * TILE]

    ours = flush(tiles, out_ref, refs[3], first) if last else []
    for u in range(min(AHEAD, len(units))):
        score(u)
    for u in range(len(units)):
        if u + AHEAD < len(units):
            score(u + AHEAD)
        soften(u)
        blend(u)
        if last:
            ours[u].start()
    for copy in copies + ours:
        copy.wait()


def attend(bias, queries, blocks, heads, before, last):
    tokens = queries.shape[0]
    operands = [bias, queries, *blocks]
    in_specs = [VMEM] * len(operands)
    span = len(blocks) * blocks[0].shape[0] - tokens + TILE
    units = len(heads) * tokens // TILE
    tile = (TILE, RATIO * HD)
    aliases = {}
    out_specs, out_shape, scratch = [], [], []
    older_heads = None
    older_units = 0
    if before is not None:
        older_heads, older, partial = before
        older_units = older.shape[0]
        operands.append(older)
        in_specs.append(VMEM)
        if partial is not None:
            aliases = {len(operands): 0}
            operands.append(in_hbm(partial))
            in_specs.append(HBM)
        out_specs.append(HBM)
        out_shape.append(pltpu.HBM((tokens, QH * HD), jnp.bfloat16))
    if last:
        scratch.append(pltpu.VMEM((units, *tile), jnp.bfloat16))
    else:
        out_specs.append(VMEM)
        out_shape.append(pltpu.VMEM((units, *tile), jnp.bfloat16))
    scratch += [
        pltpu.VMEM((AHEAD + 1, RATIO * TILE, span), jnp.float32),
        pltpu.VMEM((AHEAD + 1, RATIO * TILE, span), jnp.bfloat16),
    ]
    if last:
        scratch.append(pltpu.SemaphoreType.DMA((units,)))
    if before is not None:
        scratch.append(pltpu.SemaphoreType.DMA((older_units,)))
    return pl.pallas_call(
        functools.partial(
            attend_kernel,
            len(blocks),
            heads[0],
            None if before is None else older_heads[0],
            bool(aliases),
            last,
        ),
        in_specs=in_specs,
        out_specs=out_specs,
        out_shape=out_shape,
        scratch_shapes=scratch,
        input_output_aliases=aliases,
        compiler_params=pltpu.CompilerParams(vmem_limit_bytes=24 * MIB),
        cost_estimate=pl.CostEstimate(
            flops=6 * tokens * len(heads) * RATIO * HD * span,
            bytes_accessed=4 * tokens * len(heads) * RATIO * HD,
            transcendentals=len(heads) * RATIO * tokens * span,
        ),
        name="attend",
    )(*operands)


def shards(hidden, queries, norm_gain, kv_weight, value_bias, doc_lengths):
    return layer(hidden[0], queries[0], norm_gain, kv_weight, value_bias, doc_lengths)[None]


def layer(hidden, queries, norm_gain, kv_weight, value_bias, doc_lengths):
    tokens = hidden.shape[0]
    parts = lax.axis_size("fsdp")
    length = lax.axis_size("sp")
    held = kv_weight.shape[0]
    pair = 2 if parts % 2 == 0 else 1
    groups = parts // pair
    reach = length // 4
    gain = norm_gain[None]

    arrived = []
    for d in range(1, groups):
        there = [(i, across(i, d, parts, pair)) for i in range(parts)]
        arrived.append([])
        for p in range(PIECES):
            sent = away(hidden, gain, parts, pair, held, d, p)
            arrived[-1].append(lax.ppermute(sent, "fsdp", there))
    own, power, kept = home(hidden, gain, kv_weight, parts, pair)
    weights = [kept]
    if pair == 2:
        weights.append(lax.ppermute(kv_weight, "fsdp", [(i, i ^ 1) for i in range(parts)]))
    bias = mask(doc_lengths, tokens, reach)
    mine = project(own, weights, GROUPS, jnp.float32)

    starts = [sum(2 * len(heads) * HD for heads in GROUPS[:g]) for g in range(len(GROUPS))]
    swaps = reach % 2 == 0 and length % 2 == 0
    finished = {}
    for piece, g in CHUNKS:
        heads = GROUPS[g]
        returned = []
        for d in range(1, groups):
            back = [(across(i, d, parts, pair), i) for i in range(parts)]
            part = project(arrived[d - 1][piece], weights, [heads], jnp.bfloat16)
            returned.append(lax.ppermute(part, "fsdp", back))
        row = piece * (tokens // PIECES)
        done = merge(mine, power, value_bias[None], returned, row, starts[g], heads)
        chain = [done]
        for b in range(2, reach + 1, 2) if swaps else range(1, reach + 1):
            ahead = [(i, (i + b) % length) for i in range(length)]
            chain.append(lax.ppermute(done, "sp", ahead))
        blocks = chain
        if swaps:
            blocks = [done]
            swap = [(i, i ^ 1) for i in range(length)]
            for b in range(reach // 2):
                near = lax.ppermute(pick(chain[b], chain[b + 1]), "sp", swap)
                blocks += [near, chain[b + 1]]
        finished[piece, g] = blocks

    before = None
    for g, heads in enumerate(GROUPS):
        blocks = [finished[p, g][b] for b in range(reach, -1, -1) for p in range(PIECES)]
        last = g == len(GROUPS) - 1
        results = attend(bias, queries, blocks, heads, before, last)
        before = (heads, results[-1], results[0] if before is not None else None)
    return results[0]


def solution(mesh):
    in_specs = (
        P("fsdp", "sp", None),
        P("fsdp", "sp", None),
        P(),
        P("fsdp", None),
        P(),
        P("fsdp", None),
    )
    out_specs = P("fsdp", "sp", None)
    return jax.shard_map(shards, mesh=mesh, in_specs=in_specs, out_specs=out_specs, check_vma=False)
```
